32 devices in a mesh: narrow: 4 (over y, core), wide: 8 (over z, x).
Axes of the slice: x: 2, y: 2, z: 4, core: 2. Of those that a mesh axis runs over, the one named last changes fastest.
Arguments:
- rhs_field: float32 [2, 32768, 768], P(None, ('wide', 'narrow')), may hold values from -6 to 6
- leaf_inverse: float32 [2, 32768, 512], P(None, ('wide', 'narrow')), may hold values from -0.1875 to 0.1875
- expand_one: float32 [2, 32768, 128], P(None, ('wide', 'narrow')), may hold values from -0.375 to 0.375
- project_one: float32 [2, 32768, 128], P(None, ('wide', 'narrow')), may hold values from -0.0625 to 0.0625
- core_one: float32 [2, 1024, 256], P(None, 'wide'), may hold values from -0.25 to 0.25
- expand_two: float32 [2, 32768, 128], P(None, ('wide', 'narrow')), may hold values from -0.375 to 0.375
- project_two: float32 [2, 32768, 128], P(None, ('wide', 'narrow')), may hold values from -0.046875 to 0.046875
- core_two: float32 [2, 512, 256], replicated, may hold values from -0.25 to 0.25
- expand_three: float32 [2, 32768, 128], P(None, ('wide', 'narrow')), may hold values from -0.375 to 0.375
- project_three: float32 [2, 32768, 128], P(None, ('wide', 'narrow')), may hold values from -0.03125 to 0.03125
- core_three: float32 [2, 256, 256], replicated, may hold values from -0.25 to 0.25
Outputs:
- solution: float32 [2, 32768, 768], P(None, ('wide', 'narrow'))
The draws below stay inside these ranges and needn't reach their ends.
All inputs are finite; a program needn't handle non-finite values.
Results may differ from the reference program's by a relative error of at most 0.0003.
Values sent between devices are 32-bit elements; how exact they have to be, the bound alone decides.
No kernel may reach another device: no remote copies, remote signals or barrier semaphores. Data moves between devices by JAX's collectives and lax.ppermute only.
A program may use at most 128 MiB of HBM per device.

```python
import jax
import jax.numpy as jnp
from jax import lax

LEAF = 512
RANK = 128
NRHS = 768
ROWS_DEV = 1024
N = 32768
KIDS_ONE = 8
N_NARROW = 4
N_WIDE = 8


def steps_of(rng, extent, shards, low, top_value):
    def one(dim, shards_of):
        draws = jax.random.uniform(jax.random.fold_in(jax.random.fold_in(rng, 6), dim), (shards_of,), jnp.float32, low / len(shards), top_value / len(shards))
        return jnp.repeat(jnp.exp(draws), extent[dim] // shards_of).reshape((-1,) + (1,) * (len(extent) - dim - 1))

    gain = one(*shards[0])
    for cut in shards[1:]:
        gain = gain * one(*cut)
    return gain


def normal_values(key, dims, scale, bound, split=(), dtype=jnp.bfloat16):
    entries = jax.random.normal(key, dims, jnp.float32) * scale
    if len(split) > 0:
        entries = steps_of(key, dims, split, -0.22, 0.18) * entries
    return jnp.clip(entries, min=-bound, max=bound).astype(dtype)


def setup_inputs(seed: int = 0) -> dict:
    arg_keys = jax.random.split(jax.random.key(seed), 12)
    rhs_field = normal_values(arg_keys[0], (2, N, NRHS), 1.0, 6.0, ((1, 32),), jnp.float32)
    leaf_inverse = normal_values(arg_keys[1], (2, N, LEAF), (2 * LEAF) ** -0.5, 0.1875, ((1, 32),), jnp.float32)
    expand_one = normal_values(arg_keys[2], (2, N, RANK), (2 * RANK) ** -0.5, 0.375, ((1, 32),), jnp.float32)
    project_one = normal_values(arg_keys[3], (2, N, RANK), (2 * N_NARROW * ROWS_DEV) ** -0.5, 0.0625, ((1, 32),), jnp.float32)
    core_one = normal_values(arg_keys[4], (2, KIDS_ONE * RANK, 2 * RANK), (4 * RANK) ** -0.5, 0.25, ((1, 8),), jnp.float32)
    expand_two = normal_values(arg_keys[5], (2, N, RANK), (2 * RANK) ** -0.5, 0.375, ((1, 32),), jnp.float32)
    project_two = normal_values(arg_keys[6], (2, N, RANK), (N // 2) ** -0.5, 0.046875, ((1, 32),), jnp.float32)
    core_two = normal_values(arg_keys[7], (2, 4 * RANK, 2 * RANK), (4 * RANK) ** -0.5, 0.25, (), jnp.float32)
    expand_three = normal_values(arg_keys[8], (2, N, RANK), (2 * RANK) ** -0.5, 0.375, ((1, 32),), jnp.float32)
    project_three = normal_values(arg_keys[9], (2, N, RANK), N ** -0.5, 0.03125, ((1, 32),), jnp.float32)
    core_three = normal_values(arg_keys[10], (2, 2 * RANK, 2 * RANK), (4 * RANK) ** -0.5, 0.25, (), jnp.float32)
    return {"rhs_field": rhs_field, "leaf_inverse": leaf_inverse, "expand_one": expand_one, "project_one": project_one, "core_one": core_one, "expand_two": expand_two, "project_two": project_two, "core_two": core_two, "expand_three": expand_three, "project_three": project_three, "core_three": core_three}


def complex_product(form, first_factor, second_factor):
    highest = lax.Precision.HIGHEST
    plain = jnp.einsum(form, first_factor[0], second_factor[0], precision=highest)
    crossed = jnp.einsum(form, first_factor[1], second_factor[1], precision=highest)
    summed = jnp.einsum(form, first_factor[0] + first_factor[1], second_factor[0] + second_factor[1], precision=highest)
    return plain - crossed, summed - plain - crossed


def reference(rhs_field, leaf_inverse, expand_one, project_one, core_one, expand_two, project_two, core_two, expand_three, project_three, core_three):
    row_count = rhs_field.shape[1]
    columns = rhs_field.shape[2]
    leaves = row_count // LEAF
    inverse = leaf_inverse.reshape(2, leaves, LEAF, LEAF)
    source = rhs_field.reshape(2, leaves, LEAF, columns)
    solved = complex_product("lij,ljn->lin", (inverse[0], inverse[1]), (source[0], source[1]))
    current = (solved[0].reshape(row_count, columns), solved[1].reshape(row_count, columns))
    levels = ((expand_one, project_one, core_one, N_WIDE), (expand_two, project_two, core_two, 4), (expand_three, project_three, core_three, 2))
    for expand, project, core, children in levels:
        child_rows = row_count // children
        bases = (project[0].reshape(children, child_rows, RANK), -project[1].reshape(children, child_rows, RANK))
        pieces = (current[0].reshape(children, child_rows, columns), current[1].reshape(children, child_rows, columns))
        projected = complex_product("csr,csn->crn", bases, pieces)
        stacked = (projected[0].reshape(children // 2, 2 * RANK, columns), projected[1].reshape(children // 2, 2 * RANK, columns))
        core_blocks = (core[0].reshape(children // 2, 2 * RANK, 2 * RANK), core[1].reshape(children // 2, 2 * RANK, 2 * RANK))
        correction = complex_product("bij,bjn->bin", core_blocks, stacked)
        correction = (correction[0].reshape(children, RANK, columns), correction[1].reshape(children, RANK, columns))
        expanders = (expand[0].reshape(children, child_rows, RANK), expand[1].reshape(children, child_rows, RANK))
        update = complex_product("csr,crn->csn", expanders, correction)
        current = (current[0] - update[0].reshape(row_count, columns), current[1] - update[1].reshape(row_count, columns))
    return jnp.stack(current)
```

```python
import functools

import jax
import jax.numpy as jnp
from jax import lax
from jax.experimental import pallas as pl
from jax.experimental.pallas import tpu as pltpu
from jax.sharding import PartitionSpec as P

F32 = jnp.float32
BF16 = jnp.bfloat16
CHUNKS = 2


def swapped(array, axis, bit):
    return lax.ppermute(array, axis, [(i, i ^ 1 << bit) for i in range(lax.axis_size(axis))])


def split(value):
    high = value.astype(BF16)
    return high, (value - high.astype(F32)).astype(BF16)


def dot_nn(left, right):
    return lax.dot_general(left, right, (((1,), (0,)), ((), ())), preferred_element_type=F32)


def dot_nt(left, right):
    return lax.dot_general(left, right, (((1,), (1,)), ((), ())), preferred_element_type=F32)


def three_pass(dot, left, right):
    return dot(left[0], right[0]) + dot(left[0], right[1]) + dot(left[1], right[0])


def bits_of(size):
    return size.bit_length() - 1


def column_code():
    code = 0
    narrow = lax.axis_index("narrow")
    for bit in range(bits_of(lax.axis_size("narrow"))):
        code = code * 2 + (narrow >> bit) % 2
    return code * 2 + lax.axis_index("wide") % 2


def gram_kernel(p_two, p_three, e_one, e_two, out):
    rank = p_two.shape[2]
    left = jnp.concatenate([p_two[0].T, p_two[1].T, p_three[0].T, p_three[1].T], axis=0)
    right = jnp.concatenate([e_one[0], e_one[1], e_two[0], e_two[1]], axis=1)
    full = three_pass(dot_nn, split(left), split(right))

    def block(p, e):
        return full[p * rank : (p + 1) * rank, e * rank : (e + 1) * rank]

    pieces = []
    for p, e in ((0, 0), (1, 0), (1, 1)):
        pieces.append(block(2 * p, 2 * e) + block(2 * p + 1, 2 * e + 1))
        pieces.append(block(2 * p, 2 * e + 1) - block(2 * p + 1, 2 * e))
    both = jnp.concatenate(pieces, axis=1)
    half = rank // 2
    side = lax.axis_index("narrow") % 2

    @pl.when(side == 0)
    def _():
        out[...] = both

    @pl.when(side == 1)
    def _():
        out[:half] = both[half:]
        out[half:] = both[:half]


def leaf_kernel(blocks, inverse, source, p_one, p_two, p_three, solved, kept, sent, x_high, x_low, total):
    step = pl.program_id(0)
    per_leaf = source.shape[1] // inverse.shape[1]
    columns = source.shape[2]
    order = source.shape[1]

    @pl.when(step % per_leaf == 0)
    def _():
        for row, (first, second) in enumerate(((source[0], source[1]), (-source[1], source[0]))):
            high, low = split(jnp.concatenate([first, second], axis=1))
            x_high[row * order : (row + 1) * order] = high
            x_low[row * order : (row + 1) * order] = low

    @pl.when(step == 0)
    def _():
        total[...] = jnp.zeros_like(total)

    inverse_split = split(jnp.concatenate([inverse[0], inverse[1]], axis=1))
    y = three_pass(dot_nn, inverse_split, (x_high[...], x_low[...]))
    solved[0] = y[:, :columns]
    solved[1] = y[:, columns:]
    real_high, real_low = split(y[:, :columns].T)
    imag_high, imag_low = split(y[:, columns:].T)
    first, second = [], []
    for p in (p_one, p_two, p_three):
        first += [p[0], -p[1]]
        second += [p[1], p[0]]
    first_high, first_low = split(jnp.concatenate(first, axis=1))
    second_high, second_low = split(jnp.concatenate(second, axis=1))
    left = jnp.concatenate([real_high, imag_high, real_high, imag_high, real_low, imag_low], axis=1)
    right = jnp.concatenate([first_high, second_high, first_low, second_low, first_high, second_high], axis=0)
    total[...] += dot_nn(left, right)

    @pl.when(step == pl.num_programs(0) - 1)
    def _():
        size = columns // blocks
        code = column_code()
        for place in range(blocks):
            rows = pl.ds(pl.multiple_of((code ^ place) * size, size), size)
            target, at = (kept, place) if place < blocks // 2 else (sent, place - blocks // 2)
            target[at * size : (at + 1) * size] = total[rows]


def complex_rows(real, imag):
    return jnp.concatenate(
        [jnp.concatenate([real, -imag], axis=1), jnp.concatenate([imag, real], axis=1)], axis=0
    )


def weights_kernel(mine, other, core_one, core_two, core_three, *outs):
    rank = core_one.shape[1]
    half = rank // 2
    scratch = outs[-1]
    side = lax.axis_index("narrow") % 2
    scratch[pl.ds(pl.multiple_of(side * half, half), half)] = mine[...]
    scratch[pl.ds(pl.multiple_of((1 - side) * half, half), half)] = other[...]
    wide = lax.axis_index("wide")
    wide_bits = bits_of(lax.axis_size("wide"))
    two = wide >> (wide_bits - 2)
    three = wide >> (wide_bits - 1)

    def piece(index):
        return scratch[:, index * rank : (index + 1) * rank]

    def store(index, value):
        high, low = split(value)
        outs[2 * index][...] = high
        outs[2 * index + 1][...] = low

    def lanes(ref, part, row, child):
        at = pl.ds(pl.multiple_of(child * rank, rank), rank)
        return ref[part, row, at]

    def own_rows(child):
        return pl.ds(pl.multiple_of(child * rank, rank), rank)

    everything = slice(None)
    odd = wide % 2
    left, right = odd == 0, odd == 1
    own = [[lanes(core_one, part, everything, (odd + k) % 2) for part in range(2)] for k in range(2)]
    sib_even = [piece(12), piece(14)]
    sib_odd = [piece(13), piece(15)]
    sib_own = [jnp.where(left, a, b) for a, b in zip(sib_even, sib_odd)]
    sib_sib = [jnp.where(left, b, a) for a, b in zip(sib_even, sib_odd)]
    store(
        0,
        jnp.concatenate(
            [
                jnp.concatenate([complex_rows(*own[0]), complex_rows(*own[1])], axis=1),
                jnp.concatenate([complex_rows(*sib_own), complex_rows(*sib_sib)], axis=1),
            ],
            axis=0,
        ),
    )
    store(
        1,
        jnp.concatenate(
            [
                jnp.concatenate([complex_rows(piece(0), piece(1)), complex_rows(piece(4), piece(5))], axis=1),
                jnp.concatenate([complex_rows(piece(2), piece(3)), complex_rows(piece(6), piece(7))], axis=1),
            ],
            axis=0,
        ),
    )

    def pair(ref, rows_child, side_of):
        rows = own_rows(rows_child)
        parts = [
            complex_rows(lanes(ref, 0, rows, (side_of + k) % 2), lanes(ref, 1, rows, (side_of + k) % 2)) for k in range(2)
        ]
        return jnp.concatenate(parts, axis=1)

    store(2, jnp.concatenate([pair(core_two, two, two % 2), pair(core_two, two ^ 1, two % 2)], axis=0))
    store(3, jnp.concatenate([complex_rows(piece(8), piece(9)), complex_rows(piece(10), piece(11))], axis=1))
    store(4, pair(core_three, three, three % 2))


def first_kernel(kept, got, w_high, w_low, g_high, g_low, coefficients, rest):
    width = kept.shape[1] // 3
    stacked = jnp.concatenate([kept[:, :width], got[:, :width]], axis=1)
    solved = three_pass(dot_nt, split(stacked), (w_high[...], w_low[...]))
    coefficients[...] = solved
    rest[...] = kept[:, width:] + got[:, width:] - three_pass(dot_nt, split(solved), (g_high[...], g_low[...]))


def second_kernel(mine, got, w_high, w_low, g_high, g_low, coefficients, rest):
    width = mine.shape[1] // 2
    stacked = jnp.concatenate([mine[:, :width], got[:, :width]], axis=1)
    solved = three_pass(dot_nt, split(stacked), (w_high[...], w_low[...]))
    coefficients[...] = solved[:, :width]
    rest[...] = mine[:, width:] + got[:, width:] - three_pass(dot_nt, split(solved), (g_high[...], g_low[...]))


def third_kernel(mine, got, w_high, w_low, one, two, kept, sent):
    width = mine.shape[1]
    stacked = jnp.concatenate([mine[...], got[...]], axis=1)
    three = three_pass(dot_nt, split(stacked), (w_high[...], w_low[...]))
    kept[:, :width] = one[:, :width]
    sent[:, :width] = one[:, width:]
    for target in (kept, sent):
        target[:, width : 2 * width] = two[...]
        target[:, 2 * width :] = three


def expand_kernel(blocks, solved, kept, got, e_one, e_two, e_three, *rest):
    out, natural, w_high, w_low = rest[-4:]
    columns = solved.shape[2]
    rank = e_one.shape[2]

    @pl.when(pl.program_id(0) == 0)
    def _():
        size = columns // blocks
        code = column_code()
        for place in range(blocks):
            rows = pl.ds(pl.multiple_of((code ^ place) * size, size), size)
            source, at = (kept, place) if place < blocks // 2 else (got, place - blocks // 2)
            natural[rows] = source[at * size : (at + 1) * size]
        for level in range(natural.shape[1] // (2 * rank)):
            here = slice(2 * level * rank, (2 * level + 1) * rank)
            there = slice((2 * level + 1) * rank, (2 * level + 2) * rank)
            real_high, real_low = split(natural[:, here])
            imag_high, imag_low = split(natural[:, there])
            for target, real, imag in ((w_high, real_high, imag_high), (w_low, real_low, imag_low)):
                target[:columns, here] = real
                target[:columns, there] = -imag
                target[columns:, here] = imag
                target[columns:, there] = real

    basis = []
    for e in (e_one, e_two, e_three):
        basis += [e[0], e[1]]
    update = three_pass(dot_nt, split(jnp.concatenate(basis, axis=1)), (w_high[...], w_low[...]))
    out[0] = solved[0] - update[:, :columns]
    out[1] = solved[1] - update[:, columns:]


def shape(*dims, dtype=F32):
    return jax.ShapeDtypeStruct(dims, dtype)


def estimate(flops, moved):
    return pl.CostEstimate(flops=int(flops), bytes_accessed=int(moved), transcendentals=0)


def params(mib):
    return pltpu.CompilerParams(vmem_limit_bytes=mib * 2**20)


def body(
    rhs_field,
    leaf_inverse,
    expand_one,
    project_one,
    core_one,
    expand_two,
    project_two,
    core_two,
    expand_three,
    project_three,
    core_three,
):
    rows, columns = rhs_field.shape[1:]
    order = leaf_inverse.shape[2]
    rank = project_one.shape[2]
    half = rank // 2
    narrow_bits = bits_of(lax.axis_size("narrow"))
    wide_bits = bits_of(lax.axis_size("wide"))
    blocks = 2 ** (narrow_bits + 1)
    part = columns // CHUNKS
    tile = order // 2
    size = part // blocks
    lanes = 6 * rank

    gram = pl.pallas_call(
        gram_kernel,
        out_shape=shape(rank, lanes),
        compiler_params=params(24),
        cost_estimate=estimate(2 * 3 * 16 * rank * rank * rows, 8 * rows * rank * 4),
        name="gram",
    )(project_two, project_three, expand_one, expand_two)
    gram = gram[:half] + swapped(gram[half:], "narrow", 0)
    for bit in range(1, narrow_bits):
        gram = gram + swapped(gram, "narrow", bit)
    core_half = lax.dynamic_slice_in_dim(core_one, lax.axis_index("narrow") % 2 * half, half, 1)
    theirs = swapped(jnp.concatenate([gram, core_half[0], core_half[1]], axis=1), "wide", 0)
    summed = gram[:, 4 * rank :] + theirs[:, 4 * rank : lanes]
    for bit in range(1, wide_bits - 2):
        summed = summed + swapped(summed, "wide", bit)
    summed_theirs = swapped(summed, "wide", wide_bits - 2)
    mine = jnp.concatenate(
        [gram[:, : 4 * rank], theirs[:, : 4 * rank], summed, summed_theirs, theirs[:, lanes:]], axis=1
    )
    other = swapped(mine, "narrow", 0)
    weight_dims = ((4, 4), (4, 4), (4, 4), (2, 4), (2, 4))
    weights = pl.pallas_call(
        weights_kernel,
        out_shape=[shape(a * rank, b * rank, dtype=BF16) for a, b in weight_dims for _ in range(2)],
        scratch_shapes=[pltpu.VMEM((rank, 16 * rank), F32)],
        compiler_params=params(24),
        cost_estimate=estimate(1e6, 6e6),
        name="weights",
    )(mine, other, core_one, core_two, core_three)

    def start(chunk):
        return pl.pallas_call(
            functools.partial(leaf_kernel, blocks),
            grid=(rows // tile,),
            in_specs=[
                pl.BlockSpec((2, tile, order), lambda i: (0, i, 0)),
                pl.BlockSpec((2, order, part), lambda i: (0, i * tile // order, chunk)),
            ]
            + [pl.BlockSpec((2, tile, rank), lambda i: (0, i, 0))] * 3,
            out_specs=[
                pl.BlockSpec((2, tile, part), lambda i: (0, i, 0)),
                pl.BlockSpec((part // 2, lanes), lambda i: (0, 0)),
                pl.BlockSpec((part // 2, lanes), lambda i: (0, 0)),
            ],
            out_shape=[shape(2, rows, part), shape(part // 2, lanes), shape(part // 2, lanes)],
            scratch_shapes=[
                pltpu.VMEM((2 * order, 2 * part), BF16),
                pltpu.VMEM((2 * order, 2 * part), BF16),
                pltpu.VMEM((part, lanes), F32),
            ],
            compiler_params=params(32),
            cost_estimate=estimate(6 * rows * part * (4 * order + 12 * rank), 4 * rows * (2 * order + 2 * part)),
            name=f"leaf_{chunk}",
        )(leaf_inverse, rhs_field, project_one, project_two, project_three)

    def reduce_columns(kept, sent):
        value = kept + swapped(sent, "narrow", 0)
        for bit in range(1, narrow_bits):
            middle = value.shape[0] // 2
            value = value[:middle] + swapped(value[middle:], "narrow", bit)
        return value[:size], swapped(value[size:], "wide", 0)

    def small(kernel, name, outs, *operands):
        return pl.pallas_call(
            kernel,
            out_shape=[shape(size, width * rank) for width in outs],
            compiler_params=params(16),
            cost_estimate=estimate(2 * 6 * size * 16 * rank * rank, 4 * 16 * rank * rank),
            name=name,
        )(*operands)

    def solve(kept, got):
        one, rest = small(first_kernel, "first", (4, 4), kept, got, *weights[:4])
        for bit in range(1, wide_bits - 2):
            rest = rest + swapped(rest, "wide", bit)
        two, rest = small(second_kernel, "second", (2, 2), rest, swapped(rest, "wide", wide_bits - 2), *weights[4:8])
        return small(third_kernel, "third", (6, 6), rest, swapped(rest, "wide", wide_bits - 1), *weights[8:], one, two)

    def gather(kept, sent):
        value = jnp.concatenate([kept, swapped(sent, "wide", 0)], axis=0)
        for bit in reversed(range(1, narrow_bits)):
            value = jnp.concatenate([value, swapped(value, "narrow", bit)], axis=0)
        return value, swapped(value, "narrow", 0)

    def finish(chunk, solved, kept, got, before):
        step = order
        return pl.pallas_call(
            functools.partial(expand_kernel, blocks),
            grid=(rows // step,),
            in_specs=[
                pl.BlockSpec((2, step, part), lambda i: (0, i, 0)),
                pl.BlockSpec((part // 2, lanes), lambda i: (0, 0)),
                pl.BlockSpec((part // 2, lanes), lambda i: (0, 0)),
            ]
            + [pl.BlockSpec((2, step, rank), lambda i: (0, i, 0))] * 3
            + [pl.BlockSpec(memory_space=pl.ANY)] * len(before),
            out_specs=pl.BlockSpec((2, step, part), lambda i: (0, i, chunk)),
            out_shape=shape(2, rows, columns),
            input_output_aliases={6: 0} if before else {},
            scratch_shapes=[
                pltpu.VMEM((part, lanes), F32),
                pltpu.VMEM((2 * part, lanes), BF16),
                pltpu.VMEM((2 * part, lanes), BF16),
            ],
            compiler_params=params(32),
            cost_estimate=estimate(6 * rows * 2 * part * 6 * rank, 4 * rows * part * 4),
            name=f"expand_{chunk}",
        )(solved, kept, got, expand_one, expand_two, expand_three, *before)

    begun = [start(chunk) for chunk in range(CHUNKS)]
    out = []
    for chunk, (solved, kept, sent) in enumerate(begun):
        coefficients = gather(*solve(*reduce_columns(kept, sent)))
        out = [finish(chunk, solved, *coefficients, out)]
    return out[0]


def solution(mesh):
    placed = (
        P(None, ("wide", "narrow"), None),
        P(None, ("wide", "narrow"), None),
        P(None, ("wide", "narrow"), None),
        P(None, ("wide", "narrow"), None),
        P(None, "wide", None),
        P(None, ("wide", "narrow"), None),
        P(None, ("wide", "narrow"), None),
        P(),
        P(None, ("wide", "narrow"), None),
        P(None, ("wide", "narrow"), None),
        P(),
    )
    return jax.shard_map(
        body,
        mesh=mesh,
        in_specs=placed,
        out_specs=P(None, ("wide", "narrow"), None),
        check_vma=False,
    )
```

```python
import functools

import jax
import jax.numpy as jnp
from jax import lax
from jax.experimental import pallas as pl
from jax.experimental.pallas import tpu as pltpu
from jax.sharding import PartitionSpec as P


F32 = jnp.float32
BF16 = jnp.bfloat16
CHUNKS = 2


def swapped(array, axis, bit):
    return lax.ppermute(array, axis, [(i, i ^ 1 << bit) for i in range(lax.axis_size(axis))])


def split(value):
    high = value.astype(BF16)
    return high, (value - high.astype(F32)).astype(BF16)


def dot_nn(left, right):
    return lax.dot_general(left, right, (((1,), (0,)), ((), ())), preferred_element_type=F32)


def dot_nt(left, right):
    return lax.dot_general(left, right, (((1,), (1,)), ((), ())), preferred_element_type=F32)


def three_pass(dot, left, right):
    return dot(left[0], right[0]) + dot(left[0], right[1]) + dot(left[1], right[0])


def bits_of(size):
    return size.bit_length() - 1


def column_code():
    code = 0
    narrow = lax.axis_index("narrow")
    for bit in range(bits_of(lax.axis_size("narrow"))):
        code = code * 2 + (narrow >> bit) % 2
    return code * 2 + lax.axis_index("wide") % 2


def gram_kernel(pieces, p_two, p_three, e_one, e_two, kept, sent, held, full_two, full_three, arrived):
    rank = p_two.shape[2]
    half = rank // 2
    rows = p_two.shape[1] // pieces
    copies = [
        [
            pltpu.make_async_copy(
                array.at[:, piece * rows : (piece + 1) * rows],
                held.at[which, :, piece * rows : (piece + 1) * rows],
                arrived.at[piece, which],
            )
            for which, array in enumerate((e_one, e_two, p_two, p_three))
        ]
        for piece in range(pieces)
    ]
    for group in copies:
        for copy in group:
            copy.start()
    for piece, group in enumerate(copies):
        for copy in group:
            copy.wait()
        one, two, three, four = (
            [held[which, part, piece * rows : (piece + 1) * rows] for part in range(2)] for which in range(4)
        )
        right = split(jnp.concatenate([*one, *two], axis=1))
        near = tuple(part[:, : 2 * rank] for part in right)
        lower = three_pass(dot_nn, split(jnp.concatenate([three[0].T, three[1].T], axis=0)), near)
        upper = three_pass(dot_nn, split(jnp.concatenate([four[0].T, four[1].T], axis=0)), right)
        full_two[...] = lower if piece == 0 else full_two[...] + lower
        full_three[...] = upper if piece == 0 else full_three[...] + upper

    side = lax.axis_index("narrow") % 2
    place = 0
    for full, at in ((full_two, 0), (full_three, 0), (full_three, 2 * rank)):
        for flip in range(2):
            for target, which in ((kept, side), (sent, 1 - side)):
                upper = pl.ds(pl.multiple_of(which * half, half), half)
                lower = pl.ds(pl.multiple_of(rank + which * half, half), half)
                one = full[upper, at + flip * rank : at + (flip + 1) * rank]
                two = full[lower, at + (1 - flip) * rank : at + (2 - flip) * rank]
                target[:, place * rank : (place + 1) * rank] = one + two if flip == 0 else one - two
            place += 1


def leaf_kernel(blocks, chunk, inverse_far, source_far, one_far, two_far, three_far, *rest):
    solved, kept, sent, inverse, source, bases, x_high, x_low, total, source_in, inverse_in, bases_in = rest[-12:]
    step = pl.program_id(0)
    columns = source.shape[3]
    order = source.shape[2]
    leaves = source.shape[0]
    tiles = inverse_in.shape[0]
    tile = inverse.shape[1] // tiles
    per_leaf = tiles // leaves

    def source_copy(leaf):
        rows = pl.ds(pl.multiple_of(leaf * order, order), order)
        far = source_far.at[:, rows, chunk * columns : (chunk + 1) * columns]
        return pltpu.make_async_copy(far, source.at[leaf], source_in.at[leaf])

    def tile_copies(at):
        rows = pl.ds(pl.multiple_of(at * tile, tile), tile)
        yield pltpu.make_async_copy(inverse_far.at[:, rows], inverse.at[:, rows], inverse_in.at[at])
        for level, far in enumerate((one_far, two_far, three_far)):
            yield pltpu.make_async_copy(far.at[:, rows], bases.at[level, :, rows], bases_in.at[level, at])

    @pl.when(step == 0)
    def _():
        for at in range(tiles):
            if at % per_leaf == 0:
                source_copy(at // per_leaf).start()
            for copy in tile_copies(at):
                copy.start()

    @pl.when(step % per_leaf == 0)
    def _():
        leaf = step // per_leaf
        source_copy(leaf).wait()
        real, imag = source[leaf, 0], source[leaf, 1]
        for row, (first, second) in enumerate(((real, imag), (-imag, real))):
            high, low = split(jnp.concatenate([first, second], axis=1))
            x_high[row * order : (row + 1) * order] = high
            x_low[row * order : (row + 1) * order] = low

    for copy in tile_copies(step):
        copy.wait()
    here = pl.ds(pl.multiple_of(step * tile, tile), tile)

    @pl.when(step == 0)
    def _():
        total[...] = jnp.zeros_like(total)

    inverse_split = split(jnp.concatenate([inverse[0, here], inverse[1, here]], axis=1))
    y = three_pass(dot_nn, inverse_split, (x_high[...], x_low[...]))
    solved[0, here] = y[:, :columns]
    solved[1, here] = y[:, columns:]
    real_high, real_low = split(y[:, :columns].T)
    imag_high, imag_low = split(y[:, columns:].T)
    first, second = [], []
    for level in range(bases.shape[0]):
        real, imag = bases[level, 0, here], bases[level, 1, here]
        first += [real, -imag]
        second += [imag, real]
    first_high, first_low = split(jnp.concatenate(first, axis=1))
    second_high, second_low = split(jnp.concatenate(second, axis=1))
    left = jnp.concatenate([real_high, imag_high, real_high, imag_high, real_low, imag_low], axis=1)
    right = jnp.concatenate([first_high, second_high, first_low, second_low, first_high, second_high], axis=0)
    total[...] += dot_nn(left, right)

    @pl.when(step == pl.num_programs(0) - 1)
    def _():
        size = columns // blocks
        code = column_code()
        for place in range(blocks):
            rows = pl.ds(pl.multiple_of((code ^ place) * size, size), size)
            target, at = (kept, place) if place < blocks // 2 else (sent, place - blocks // 2)
            target[at * size : (at + 1) * size] = total[rows]


def complex_rows(real, imag):
    return jnp.concatenate(
        [jnp.concatenate([real, -imag], axis=1), jnp.concatenate([imag, real], axis=1)], axis=0
    )


def weights_kernel(mine, other, core_one, core_two, core_three, *outs):
    rank = core_one.shape[1]
    half = rank // 2
    scratch = outs[-1]
    side = lax.axis_index("narrow") % 2
    scratch[pl.ds(pl.multiple_of(side * half, half), half)] = mine[...]
    scratch[pl.ds(pl.multiple_of((1 - side) * half, half), half)] = other[...]
    wide = lax.axis_index("wide")
    wide_bits = bits_of(lax.axis_size("wide"))
    two = wide >> (wide_bits - 2)
    three = wide >> (wide_bits - 1)

    def piece(index):
        return scratch[:, index * rank : (index + 1) * rank]

    def store(index, value):
        high, low = split(value)
        outs[2 * index][...] = high
        outs[2 * index + 1][...] = low

    def lanes(ref, part, row, child):
        at = pl.ds(pl.multiple_of(child * rank, rank), rank)
        return ref[part, row, at]

    def own_rows(child):
        return pl.ds(pl.multiple_of(child * rank, rank), rank)

    everything = slice(None)
    odd = wide % 2
    left = odd == 0
    own = [[lanes(core_one, part, everything, (odd + k) % 2) for part in range(2)] for k in range(2)]
    sib_even = [piece(12), piece(14)]
    sib_odd = [piece(13), piece(15)]
    sib_own = [jnp.where(left, a, b) for a, b in zip(sib_even, sib_odd)]
    sib_sib = [jnp.where(left, b, a) for a, b in zip(sib_even, sib_odd)]
    store(
        0,
        jnp.concatenate(
            [
                jnp.concatenate([complex_rows(*own[0]), complex_rows(*own[1])], axis=1),
                jnp.concatenate([complex_rows(*sib_own), complex_rows(*sib_sib)], axis=1),
            ],
            axis=0,
        ),
    )
    store(
        1,
        jnp.concatenate(
            [
                jnp.concatenate([complex_rows(piece(0), piece(1)), complex_rows(piece(4), piece(5))], axis=1),
                jnp.concatenate([complex_rows(piece(2), piece(3)), complex_rows(piece(6), piece(7))], axis=1),
            ],
            axis=0,
        ),
    )

    def pair(ref, rows_child, side_of):
        rows = own_rows(rows_child)
        parts = [
            complex_rows(lanes(ref, 0, rows, (side_of + k) % 2), lanes(ref, 1, rows, (side_of + k) % 2)) for k in range(2)
        ]
        return jnp.concatenate(parts, axis=1)

    store(2, jnp.concatenate([pair(core_two, two, two % 2), pair(core_two, two ^ 1, two % 2)], axis=0))
    store(3, jnp.concatenate([complex_rows(piece(8), piece(9)), complex_rows(piece(10), piece(11))], axis=1))
    store(4, pair(core_three, three, three % 2))


def first_kernel(kept, got, w_high, w_low, g_high, g_low, coefficients, rest):
    width = kept.shape[1] // 3
    stacked = jnp.concatenate([kept[:, :width], got[:, :width]], axis=1)
    solved = three_pass(dot_nt, split(stacked), (w_high[...], w_low[...]))
    coefficients[...] = solved
    rest[...] = kept[:, width:] + got[:, width:] - three_pass(dot_nt, split(solved), (g_high[...], g_low[...]))


def second_kernel(mine, got, w_high, w_low, g_high, g_low, coefficients, rest):
    width = mine.shape[1] // 2
    stacked = jnp.concatenate([mine[:, :width], got[:, :width]], axis=1)
    solved = three_pass(dot_nt, split(stacked), (w_high[...], w_low[...]))
    coefficients[...] = solved[:, :width]
    rest[...] = mine[:, width:] + got[:, width:] - three_pass(dot_nt, split(solved), (g_high[...], g_low[...]))


def third_kernel(mine, got, w_high, w_low, one, two, kept, sent):
    width = mine.shape[1]
    stacked = jnp.concatenate([mine[...], got[...]], axis=1)
    three = three_pass(dot_nt, split(stacked), (w_high[...], w_low[...]))
    kept[:, :width] = one[:, :width]
    sent[:, :width] = one[:, width:]
    for target in (kept, sent):
        target[:, width : 2 * width] = two[...]
        target[:, 2 * width :] = three


def expand_kernel(blocks, solved, kept, got, e_one, e_two, e_three, *rest):
    out, natural, w_high, w_low = rest[-4:]
    columns = solved.shape[2]
    rank = e_one.shape[2]

    @pl.when(pl.program_id(0) == 0)
    def _():
        size = columns // blocks
        code = column_code()
        for place in range(blocks):
            rows = pl.ds(pl.multiple_of((code ^ place) * size, size), size)
            source, at = (kept, place) if place < blocks // 2 else (got, place - blocks // 2)
            natural[rows] = source[at * size : (at + 1) * size]
        for level in range(natural.shape[1] // (2 * rank)):
            here = slice(2 * level * rank, (2 * level + 1) * rank)
            there = slice((2 * level + 1) * rank, (2 * level + 2) * rank)
            real_high, real_low = split(natural[:, here])
            imag_high, imag_low = split(natural[:, there])
            for target, real, imag in ((w_high, real_high, imag_high), (w_low, real_low, imag_low)):
                target[:columns, here] = real
                target[:columns, there] = -imag
                target[columns:, here] = imag
                target[columns:, there] = real

    basis = []
    for e in (e_one, e_two, e_three):
        basis += [e[0], e[1]]
    update = three_pass(dot_nt, split(jnp.concatenate(basis, axis=1)), (w_high[...], w_low[...]))
    out[0] = solved[0] - update[:, :columns]
    out[1] = solved[1] - update[:, columns:]


def shape(*dims, dtype=F32):
    return jax.ShapeDtypeStruct(dims, dtype)


def estimate(flops, moved):
    return pl.CostEstimate(flops=int(flops), bytes_accessed=int(moved), transcendentals=0)


def params(mib):
    return pltpu.CompilerParams(vmem_limit_bytes=mib * 2**20)


def body(
    rhs_field,
    leaf_inverse,
    expand_one,
    project_one,
    core_one,
    expand_two,
    project_two,
    core_two,
    expand_three,
    project_three,
    core_three,
):
    def far_only(*arrays):
        return [pltpu.with_memory_space_constraint(array, pltpu.HBM) for array in arrays]

    rows, columns = rhs_field.shape[1:]
    order = leaf_inverse.shape[2]
    rank = project_one.shape[2]
    half = rank // 2
    narrow_bits = bits_of(lax.axis_size("narrow"))
    wide_bits = bits_of(lax.axis_size("wide"))
    blocks = 2 ** (narrow_bits + 1)
    part = columns // CHUNKS
    tile = order
    size = part // blocks
    lanes = 6 * rank

    far = pl.BlockSpec(memory_space=pltpu.HBM)

    def start(chunk, *after):
        return pl.pallas_call(
            functools.partial(leaf_kernel, blocks, chunk),
            grid=(rows // tile,),
            in_specs=[far] * 5 + [pl.BlockSpec(memory_space=pl.ANY)] * len(after),
            out_specs=[
                pl.BlockSpec((2, rows, part), lambda i: (0, 0, 0)),
                pl.BlockSpec((part // 2, lanes), lambda i: (0, 0)),
                pl.BlockSpec((part // 2, lanes), lambda i: (0, 0)),
            ],
            out_shape=[shape(2, rows, part), shape(part // 2, lanes), shape(part // 2, lanes)],
            scratch_shapes=[
                pltpu.VMEM((2, rows, order), F32),
                pltpu.VMEM((rows // order, 2, order, part), F32),
                pltpu.VMEM((3, 2, rows, rank), F32),
                pltpu.VMEM((2 * order, 2 * part), BF16),
                pltpu.VMEM((2 * order, 2 * part), BF16),
                pltpu.VMEM((part, lanes), F32),
                pltpu.SemaphoreType.DMA((rows // order,)),
                pltpu.SemaphoreType.DMA((rows // tile,)),
                pltpu.SemaphoreType.DMA((3, rows // tile)),
            ],
            compiler_params=params(40),
            cost_estimate=estimate(6 * rows * part * (4 * order + 12 * rank), 4 * rows * (2 * order + 2 * part)),
        )(*far_only(leaf_inverse, rhs_field, project_one, project_two, project_three), *after)

    def small(kernel, outs, after, *operands):
        def run(*refs):
            kernel(*refs[: len(operands)], *refs[len(operands) + len(after) :])

        return pl.pallas_call(
            run,
            in_specs=[pl.BlockSpec(memory_space=pltpu.VMEM)] * len(operands)
            + [pl.BlockSpec(memory_space=pl.ANY)] * len(after),
            out_shape=[shape(size, width * rank) for width in outs],
            compiler_params=params(16),
            cost_estimate=estimate(2 * 6 * size * 16 * rank * rank, 4 * 16 * rank * rank),
        )(*operands, *after)

    def columns_step(value, bit):
        middle = value.shape[0] // 2
        return value[:middle] + swapped(value[middle:], "narrow", bit)

    def first(value):
        kept, got = value[:size], swapped(value[size:], "wide", 0)
        return small(first_kernel, (4, 4), (), kept, got, *weights[:4])

    def second(rest, after):
        for bit in range(1, wide_bits - 2):
            rest = rest + swapped(rest, "wide", bit)
        got = swapped(rest, "wide", wide_bits - 2)
        return small(second_kernel, (2, 2), after, rest, got, *weights[4:8])

    def third(one, two, rest, after):
        got = swapped(rest, "wide", wide_bits - 1)
        return small(third_kernel, (6, 6), after, rest, got, *weights[8:], one, two)

    def grown(kept, got):
        return jnp.concatenate([kept, got], axis=0)

    def finish(chunk, solved, kept, got, before):
        step = order
        return pl.pallas_call(
            functools.partial(expand_kernel, blocks),
            grid=(rows // step,),
            in_specs=[
                pl.BlockSpec((2, step, part), lambda i: (0, i, 0)),
                pl.BlockSpec((part // 2, lanes), lambda i: (0, 0)),
                pl.BlockSpec((part // 2, lanes), lambda i: (0, 0)),
            ]
            + [pl.BlockSpec((2, step, rank), lambda i: (0, i, 0))] * 3
            + [pl.BlockSpec(memory_space=pl.ANY)] * len(before),
            out_specs=pl.BlockSpec((2, step, part), lambda i: (0, i, chunk)),
            out_shape=shape(2, rows, columns),
            input_output_aliases={6: 0} if before else {},
            scratch_shapes=[
                pltpu.VMEM((part, lanes), F32),
                pltpu.VMEM((2 * part, lanes), BF16),
                pltpu.VMEM((2 * part, lanes), BF16),
            ],
            compiler_params=params(32),
            cost_estimate=estimate(6 * rows * 2 * part * 6 * rank, 4 * rows * part * 4),
        )(solved, kept, got, expand_one, expand_two, expand_three, *before)

    half_gram = shape(half, lanes)
    pieces = 4
    gram, gram_sent = pl.pallas_call(
        functools.partial(gram_kernel, pieces),
        in_specs=[far] * 4,
        out_shape=[half_gram, half_gram],
        scratch_shapes=[
            pltpu.VMEM((4, 2, rows, rank), F32),
            pltpu.VMEM((2 * rank, 2 * rank), F32),
            pltpu.VMEM((2 * rank, 4 * rank), F32),
            pltpu.SemaphoreType.DMA((pieces, 4)),
        ],
        compiler_params=params(20),
        cost_estimate=estimate(2 * 3 * 12 * rank * rank * rows, 8 * rows * rank * 4),
        name="gram",
    )(*far_only(project_two, project_three, expand_one, expand_two))
    gram = gram + swapped(gram_sent, "narrow", 0)
    solved_a, kept, sent = start(0, gram)
    for bit in range(1, narrow_bits):
        gram = gram + swapped(gram, "narrow", bit)
    core_half = lax.dynamic_slice_in_dim(core_one, lax.axis_index("narrow") % 2 * half, half, 1)
    theirs = swapped(jnp.concatenate([gram, core_half[0], core_half[1]], axis=1), "wide", 0)
    a = kept + swapped(sent, "narrow", 0)
    solved_b, kept, sent = start(1, a, gram)
    for bit in range(1, narrow_bits):
        a = columns_step(a, bit)
    summed = gram[:, 4 * rank :] + theirs[:, 4 * rank : lanes]
    for bit in range(1, wide_bits - 2):
        summed = summed + swapped(summed, "wide", bit)
    summed_theirs = swapped(summed, "wide", wide_bits - 2)
    mine = jnp.concatenate(
        [gram[:, : 4 * rank], theirs[:, : 4 * rank], summed, summed_theirs, theirs[:, lanes:]], axis=1
    )
    other = swapped(mine, "narrow", 0)
    b = kept + swapped(sent, "narrow", 0)
    weight_dims = ((4, 4), (4, 4), (4, 4), (2, 4), (2, 4))
    weights = pl.pallas_call(
        weights_kernel,
        out_shape=[shape(a * rank, b * rank, dtype=BF16) for a, b in weight_dims for _ in range(2)],
        scratch_shapes=[pltpu.VMEM((rank, 16 * rank), F32)],
        compiler_params=params(24),
        cost_estimate=estimate(1e6, 6e6),
        name="weights",
    )(mine, other, core_one, core_two, core_three)

    one_a, a = first(a)
    for bit in range(1, narrow_bits):
        b = columns_step(b, bit)
    two_a, a = second(a, ())
    a, a_sent = third(one_a, two_a, a, ())
    one_b, b = first(b)
    a = grown(a, swapped(a_sent, "wide", 0))
    two_b, b = second(b, ())
    for bit in reversed(range(1, narrow_bits)):
        a = grown(a, swapped(a, "narrow", bit))
    b, b_sent = third(one_b, two_b, b, ())
    b = grown(b, swapped(b_sent, "wide", 0))
    out = finish(0, solved_a, a, swapped(a, "narrow", 0), [])
    for bit in reversed(range(1, narrow_bits)):
        b = grown(b, swapped(b, "narrow", bit))
    return finish(1, solved_b, b, swapped(b, "narrow", 0), [out])


def solution(mesh):
    placed = (
        P(None, ("wide", "narrow"), None),
        P(None, ("wide", "narrow"), None),
        P(None, ("wide", "narrow"), None),
        P(None, ("wide", "narrow"), None),
        P(None, "wide", None),
        P(None, ("wide", "narrow"), None),
        P(None, ("wide", "narrow"), None),
        P(),
        P(None, ("wide", "narrow"), None),
        P(None, ("wide", "narrow"), None),
        P(),
    )

    return jax.shard_map(
        body,
        mesh=mesh,
        in_specs=placed,
        out_specs=P(None, ("wide", "narrow"), None),
        check_vma=False,
    )
```

```python
import functools

import jax
import jax.numpy as jnp
from jax import lax
from jax.experimental import pallas as pl
from jax.experimental.pallas import tpu as pltpu
from jax.sharding import PartitionSpec as P


F32 = jnp.float32
BF16 = jnp.bfloat16
CHUNKS = 2


def swapped(array, axis, bit):
    return lax.ppermute(array, axis, [(i, i ^ 1 << bit) for i in range(lax.axis_size(axis))])


def split(value):
    high = value.astype(BF16)
    return high, (value - high.astype(F32)).astype(BF16)


def dot_nn(left, right):
    return lax.dot_general(left, right, (((1,), (0,)), ((), ())), preferred_element_type=F32)


def dot_nt(left, right):
    return lax.dot_general(left, right, (((1,), (1,)), ((), ())), preferred_element_type=F32)


def three_pass(dot, left, right):
    return dot(left[0], right[0]) + dot(left[0], right[1]) + dot(left[1], right[0])


def bits_of(size):
    return size.bit_length() - 1


def column_code():
    code = 0
    narrow = lax.axis_index("narrow")
    for bit in range(bits_of(lax.axis_size("narrow"))):
        code = code * 2 + (narrow >> bit) % 2
    return code * 2 + lax.axis_index("wide") % 2


def gram_kernel(pieces, p_two, p_three, e_one, e_two, kept, sent, held, full_two, full_three, arrived):
    rank = p_two.shape[2]
    half = rank // 2
    rows = p_two.shape[1] // pieces
    copies = [
        [
            pltpu.make_async_copy(
                array.at[:, piece * rows : (piece + 1) * rows],
                held.at[which, :, piece * rows : (piece + 1) * rows],
                arrived.at[piece, which],
            )
            for which, array in enumerate((e_one, e_two, p_two, p_three))
        ]
        for piece in range(pieces)
    ]
    for group in copies:
        for copy in group:
            copy.start()
    for piece, group in enumerate(copies):
        for copy in group:
            copy.wait()
        one, two, three, four = (
            [held[which, part, piece * rows : (piece + 1) * rows] for part in range(2)] for which in range(4)
        )
        right = split(jnp.concatenate([*one, *two], axis=1))
        near = tuple(part[:, : 2 * rank] for part in right)
        lower = three_pass(dot_nn, split(jnp.concatenate([three[0].T, three[1].T], axis=0)), near)
        upper = three_pass(dot_nn, split(jnp.concatenate([four[0].T, four[1].T], axis=0)), right)
        full_two[...] = lower if piece == 0 else full_two[...] + lower
        full_three[...] = upper if piece == 0 else full_three[...] + upper

    side = lax.axis_index("narrow") % 2
    place = 0
    for full, at in ((full_two, 0), (full_three, 0), (full_three, 2 * rank)):
        for flip in range(2):
            for target, which in ((kept, side), (sent, 1 - side)):
                upper = pl.ds(pl.multiple_of(which * half, half), half)
                lower = pl.ds(pl.multiple_of(rank + which * half, half), half)
                one = full[upper, at + flip * rank : at + (flip + 1) * rank]
                two = full[lower, at + (1 - flip) * rank : at + (2 - flip) * rank]
                target[:, place * rank : (place + 1) * rank] = one + two if flip == 0 else one - two
            place += 1


def leaf_kernel(blocks, chunk, inverse_far, source_far, one_far, two_far, three_far, *rest):
    solved, kept, sent, inverse, source, bases, x_high, x_low, total, source_in, inverse_in, bases_in = rest[-12:]
    step = pl.program_id(0)
    columns = source.shape[3]
    order = source.shape[2]
    leaves = source.shape[0]
    tiles = inverse_in.shape[0]
    tile = inverse.shape[1] // tiles
    per_leaf = tiles // leaves

    def source_copy(leaf):
        rows = pl.ds(pl.multiple_of(leaf * order, order), order)
        far = source_far.at[:, rows, chunk * columns : (chunk + 1) * columns]
        return pltpu.make_async_copy(far, source.at[leaf], source_in.at[leaf])

    def tile_copies(at):
        rows = pl.ds(pl.multiple_of(at * tile, tile), tile)
        yield pltpu.make_async_copy(inverse_far.at[:, rows], inverse.at[:, rows], inverse_in.at[at])
        for level, far in enumerate((one_far, two_far, three_far)):
            yield pltpu.make_async_copy(far.at[:, rows], bases.at[level, :, rows], bases_in.at[level, at])

    @pl.when(step == 0)
    def _():
        for at in range(tiles):
            if at % per_leaf == 0:
                source_copy(at // per_leaf).start()
            for copy in tile_copies(at):
                copy.start()

    @pl.when(step % per_leaf == 0)
    def _():
        leaf = step // per_leaf
        source_copy(leaf).wait()
        real, imag = source[leaf, 0], source[leaf, 1]
        for row, (first, second) in enumerate(((real, imag), (-imag, real))):
            high, low = split(jnp.concatenate([first, second], axis=1))
            x_high[row * order : (row + 1) * order] = high
            x_low[row * order : (row + 1) * order] = low

    for copy in tile_copies(step):
        copy.wait()
    here = pl.ds(pl.multiple_of(step * tile, tile), tile)

    @pl.when(step == 0)
    def _():
        total[...] = jnp.zeros_like(total)

    inverse_split = split(jnp.concatenate([inverse[0, here], inverse[1, here]], axis=1))
    y = three_pass(dot_nn, inverse_split, (x_high[...], x_low[...]))
    solved[0, here] = y[:, :columns]
    solved[1, here] = y[:, columns:]
    real_high, real_low = split(y[:, :columns].T)
    imag_high, imag_low = split(y[:, columns:].T)
    first, second = [], []
    for level in range(bases.shape[0]):
        real, imag = bases[level, 0, here], bases[level, 1, here]
        first += [real, -imag]
        second += [imag, real]
    first_high, first_low = split(jnp.concatenate(first, axis=1))
    second_high, second_low = split(jnp.concatenate(second, axis=1))
    left = jnp.concatenate([real_high, imag_high, real_high, imag_high, real_low, imag_low], axis=1)
    right = jnp.concatenate([first_high, second_high, first_low, second_low, first_high, second_high], axis=0)
    total[...] += dot_nn(left, right)

    @pl.when(step == pl.num_programs(0) - 1)
    def _():
        size = columns // blocks
        code = column_code()
        for place in range(blocks):
            rows = pl.ds(pl.multiple_of((code ^ place) * size, size), size)
            target, at = (kept, place) if place < blocks // 2 else (sent, place - blocks // 2)
            target[at * size : (at + 1) * size] = total[rows]


def complex_rows(real, imag):
    return jnp.concatenate(
        [jnp.concatenate([real, -imag], axis=1), jnp.concatenate([imag, real], axis=1)], axis=0
    )


def joined(mine, other, whole):
    half = mine.shape[0]
    side = lax.axis_index("narrow") % 2
    whole[pl.ds(pl.multiple_of(side * half, half), half)] = mine[...]
    whole[pl.ds(pl.multiple_of((1 - side) * half, half), half)] = other[...]


def store(high_ref, low_ref, value):
    high_ref[...], low_ref[...] = split(value)


def lane_block(ref, part, rows, child, rank):
    return ref[part, rows, pl.ds(pl.multiple_of(child * rank, rank), rank)]


def near_weights_kernel(mine, other, core_one, core_high, core_low, gram_high, gram_low, whole):
    rank = core_one.shape[1]
    joined(mine, other, whole)
    odd = lax.axis_index("wide") % 2

    def piece(index):
        return whole[:, index * rank : (index + 1) * rank]

    own = [[lane_block(core_one, part, slice(None), (odd + k) % 2, rank) for part in range(2)] for k in range(2)]
    even_first = odd == 0
    sib_own = [jnp.where(even_first, piece(8 + 2 * part), piece(9 + 2 * part)) for part in range(2)]
    sib_sib = [jnp.where(even_first, piece(9 + 2 * part), piece(8 + 2 * part)) for part in range(2)]
    upper = jnp.concatenate([complex_rows(*own[0]), complex_rows(*own[1])], axis=1)
    lower = jnp.concatenate([complex_rows(*sib_own), complex_rows(*sib_sib)], axis=1)
    store(core_high, core_low, jnp.concatenate([upper, lower], axis=0))
    upper = jnp.concatenate([complex_rows(piece(0), piece(1)), complex_rows(piece(4), piece(5))], axis=1)
    lower = jnp.concatenate([complex_rows(piece(2), piece(3)), complex_rows(piece(6), piece(7))], axis=1)
    store(gram_high, gram_low, jnp.concatenate([upper, lower], axis=0))


def far_weights_kernel(mine, other, core_two, core_three, *outs):
    whole = outs[-1]
    rank = whole.shape[0]
    joined(mine, other, whole)
    wide = lax.axis_index("wide")
    wide_bits = bits_of(lax.axis_size("wide"))
    two = wide >> (wide_bits - 2)
    three = wide >> (wide_bits - 1)

    def piece(index):
        return whole[:, index * rank : (index + 1) * rank]

    def pair(ref, child, side):
        rows = pl.ds(pl.multiple_of(child * rank, rank), rank)
        parts = [[lane_block(ref, part, rows, (side + k) % 2, rank) for part in range(2)] for k in range(2)]
        return jnp.concatenate([complex_rows(*parts[0]), complex_rows(*parts[1])], axis=1)

    store(outs[0], outs[1], jnp.concatenate([pair(core_two, two, two % 2), pair(core_two, two ^ 1, two % 2)], axis=0))
    store(outs[2], outs[3], jnp.concatenate([complex_rows(piece(0), piece(1)), complex_rows(piece(2), piece(3))], axis=1))
    store(outs[4], outs[5], pair(core_three, three, three % 2))


def first_kernel(kept, got, w_high, w_low, g_high, g_low, coefficients, rest):
    width = kept.shape[1] // 3
    stacked = jnp.concatenate([kept[:, :width], got[:, :width]], axis=1)
    solved = three_pass(dot_nt, split(stacked), (w_high[...], w_low[...]))
    coefficients[...] = solved
    rest[...] = kept[:, width:] + got[:, width:] - three_pass(dot_nt, split(solved), (g_high[...], g_low[...]))


def second_kernel(mine, got, w_high, w_low, g_high, g_low, coefficients, rest):
    width = mine.shape[1] // 2
    stacked = jnp.concatenate([mine[:, :width], got[:, :width]], axis=1)
    solved = three_pass(dot_nt, split(stacked), (w_high[...], w_low[...]))
    coefficients[...] = solved[:, :width]
    rest[...] = mine[:, width:] + got[:, width:] - three_pass(dot_nt, split(solved), (g_high[...], g_low[...]))


def third_kernel(mine, got, w_high, w_low, one, two, kept, sent):
    width = mine.shape[1]
    stacked = jnp.concatenate([mine[...], got[...]], axis=1)
    three = three_pass(dot_nt, split(stacked), (w_high[...], w_low[...]))
    kept[:, :width] = one[:, :width]
    sent[:, :width] = one[:, width:]
    for target in (kept, sent):
        target[:, width : 2 * width] = two[...]
        target[:, 2 * width :] = three


def expand_kernel(blocks, solved, kept, got, e_one, e_two, e_three, *rest):
    out, natural, w_high, w_low = rest[-4:]
    columns = solved.shape[2]
    rank = e_one.shape[2]

    @pl.when(pl.program_id(0) == 0)
    def _():
        size = columns // blocks
        code = column_code()
        for place in range(blocks):
            rows = pl.ds(pl.multiple_of((code ^ place) * size, size), size)
            source, at = (kept, place) if place < blocks // 2 else (got, place - blocks // 2)
            natural[rows] = source[at * size : (at + 1) * size]
        for level in range(natural.shape[1] // (2 * rank)):
            here = slice(2 * level * rank, (2 * level + 1) * rank)
            there = slice((2 * level + 1) * rank, (2 * level + 2) * rank)
            real_high, real_low = split(natural[:, here])
            imag_high, imag_low = split(natural[:, there])
            for target, real, imag in ((w_high, real_high, imag_high), (w_low, real_low, imag_low)):
                target[:columns, here] = real
                target[:columns, there] = -imag
                target[columns:, here] = imag
                target[columns:, there] = real

    basis = []
    for e in (e_one, e_two, e_three):
        basis += [e[0], e[1]]
    update = three_pass(dot_nt, split(jnp.concatenate(basis, axis=1)), (w_high[...], w_low[...]))
    out[0] = solved[0] - update[:, :columns]
    out[1] = solved[1] - update[:, columns:]


def shape(*dims, dtype=F32):
    return jax.ShapeDtypeStruct(dims, dtype)


def estimate(flops, moved):
    return pl.CostEstimate(flops=int(flops), bytes_accessed=int(moved), transcendentals=0)


def params(mib):
    return pltpu.CompilerParams(vmem_limit_bytes=mib * 2**20)


def body(
    rhs_field,
    leaf_inverse,
    expand_one,
    project_one,
    core_one,
    expand_two,
    project_two,
    core_two,
    expand_three,
    project_three,
    core_three,
):
    def far_only(*arrays):
        return [pltpu.with_memory_space_constraint(array, pltpu.HBM) for array in arrays]

    rows, columns = rhs_field.shape[1:]
    order = leaf_inverse.shape[2]
    rank = project_one.shape[2]
    half = rank // 2
    narrow_bits = bits_of(lax.axis_size("narrow"))
    wide_bits = bits_of(lax.axis_size("wide"))
    blocks = 2 ** (narrow_bits + 1)
    part = columns // CHUNKS
    tile = order
    size = part // blocks
    lanes = 6 * rank

    far = pl.BlockSpec(memory_space=pltpu.HBM)

    def start(chunk, *after):
        return pl.pallas_call(
            functools.partial(leaf_kernel, blocks, chunk),
            grid=(rows // tile,),
            in_specs=[far] * 5 + [pl.BlockSpec(memory_space=pl.ANY)] * len(after),
            out_specs=[
                pl.BlockSpec((2, rows, part), lambda i: (0, 0, 0)),
                pl.BlockSpec((part // 2, lanes), lambda i: (0, 0)),
                pl.BlockSpec((part // 2, lanes), lambda i: (0, 0)),
            ],
            out_shape=[shape(2, rows, part), shape(part // 2, lanes), shape(part // 2, lanes)],
            scratch_shapes=[
                pltpu.VMEM((2, rows, order), F32),
                pltpu.VMEM((rows // order, 2, order, part), F32),
                pltpu.VMEM((3, 2, rows, rank), F32),
                pltpu.VMEM((2 * order, 2 * part), BF16),
                pltpu.VMEM((2 * order, 2 * part), BF16),
                pltpu.VMEM((part, lanes), F32),
                pltpu.SemaphoreType.DMA((rows // order,)),
                pltpu.SemaphoreType.DMA((rows // tile,)),
                pltpu.SemaphoreType.DMA((3, rows // tile)),
            ],
            compiler_params=params(40),
            cost_estimate=estimate(6 * rows * part * (4 * order + 12 * rank), 4 * rows * (2 * order + 2 * part)),
        )(*far_only(leaf_inverse, rhs_field, project_one, project_two, project_three), *after)

    def small(kernel, outs, after, *operands):
        def run(*refs):
            kernel(*refs[: len(operands)], *refs[len(operands) + len(after) :])

        return pl.pallas_call(
            run,
            in_specs=[pl.BlockSpec(memory_space=pltpu.VMEM)] * len(operands)
            + [pl.BlockSpec(memory_space=pl.ANY)] * len(after),
            out_shape=[shape(size, width * rank) for width in outs],
            compiler_params=params(16),
            cost_estimate=estimate(2 * 6 * size * 16 * rank * rank, 4 * 16 * rank * rank),
        )(*operands, *after)

    def columns_step(value, bit):
        middle = value.shape[0] // 2
        return value[:middle] + swapped(value[middle:], "narrow", bit)

    def first(value):
        kept, got = value[:size], swapped(value[size:], "wide", 0)
        return small(first_kernel, (4, 4), (), kept, got, *weights[:4])

    def second(rest, after):
        for bit in range(1, wide_bits - 2):
            rest = rest + swapped(rest, "wide", bit)
        got = swapped(rest, "wide", wide_bits - 2)
        return small(second_kernel, (2, 2), after, rest, got, *weights[4:8])

    def third(one, two, rest, after):
        got = swapped(rest, "wide", wide_bits - 1)
        return small(third_kernel, (6, 6), after, rest, got, *weights[8:], one, two)

    def grown(kept, got):
        return jnp.concatenate([kept, got], axis=0)

    def finish(chunk, solved, kept, got, before):
        step = order
        return pl.pallas_call(
            functools.partial(expand_kernel, blocks),
            grid=(rows // step,),
            in_specs=[
                pl.BlockSpec((2, step, part), lambda i: (0, i, 0)),
                pl.BlockSpec((part // 2, lanes), lambda i: (0, 0)),
                pl.BlockSpec((part // 2, lanes), lambda i: (0, 0)),
            ]
            + [pl.BlockSpec((2, step, rank), lambda i: (0, i, 0))] * 3
            + [pl.BlockSpec(memory_space=pl.ANY)] * len(before),
            out_specs=pl.BlockSpec((2, step, part), lambda i: (0, i, chunk)),
            out_shape=shape(2, rows, columns),
            input_output_aliases={6: 0} if before else {},
            scratch_shapes=[
                pltpu.VMEM((part, lanes), F32),
                pltpu.VMEM((2 * part, lanes), BF16),
                pltpu.VMEM((2 * part, lanes), BF16),
            ],
            compiler_params=params(32),
            cost_estimate=estimate(6 * rows * 2 * part * 6 * rank, 4 * rows * part * 4),
        )(solved, kept, got, expand_one, expand_two, expand_three, *before)

    half_gram = shape(half, lanes)
    pieces = 4
    gram, gram_sent = pl.pallas_call(
        functools.partial(gram_kernel, pieces),
        in_specs=[far] * 4,
        out_shape=[half_gram, half_gram],
        scratch_shapes=[
            pltpu.VMEM((4, 2, rows, rank), F32),
            pltpu.VMEM((2 * rank, 2 * rank), F32),
            pltpu.VMEM((2 * rank, 4 * rank), F32),
            pltpu.SemaphoreType.DMA((pieces, 4)),
        ],
        compiler_params=params(20),
        cost_estimate=estimate(2 * 3 * 12 * rank * rank * rows, 8 * rows * rank * 4),
        name="gram",
    )(*far_only(project_two, project_three, expand_one, expand_two))
    gram = gram + swapped(gram_sent, "narrow", 0)
    solved_a, kept, sent = start(0, gram)
    for bit in range(1, narrow_bits):
        gram = gram + swapped(gram, "narrow", bit)
    core_half = lax.dynamic_slice_in_dim(core_one, lax.axis_index("narrow") % 2 * half, half, 1)
    theirs = swapped(jnp.concatenate([gram, core_half[0], core_half[1]], axis=1), "wide", 0)
    a = kept + swapped(sent, "narrow", 0)
    solved_b, kept, sent = start(1, a, gram)
    for bit in range(1, narrow_bits):
        a = columns_step(a, bit)
    b = kept + swapped(sent, "narrow", 0)

    def weights_of(kernel, dims, blocks_held, *operands):
        return pl.pallas_call(
            kernel,
            out_shape=[shape(i * rank, j * rank, dtype=BF16) for i, j in dims for _ in range(2)],
            scratch_shapes=[pltpu.VMEM((rank, blocks_held * rank), F32)],
            compiler_params=params(24),
            cost_estimate=estimate(1e6, 3e6),
        )(*operands)

    mine = jnp.concatenate([gram[:, : 4 * rank], theirs[:, : 4 * rank], theirs[:, lanes:]], axis=1)
    near = weights_of(near_weights_kernel, ((4, 4), (4, 4)), 12, mine, swapped(mine, "narrow", 0), core_one)
    summed = gram[:, 4 * rank :] + theirs[:, 4 * rank : lanes]
    for bit in range(1, wide_bits - 2):
        summed = summed + swapped(summed, "wide", bit)
    mine = jnp.concatenate([summed, swapped(summed, "wide", wide_bits - 2)], axis=1)
    other = swapped(mine, "narrow", 0)
    coarse = weights_of(far_weights_kernel, ((4, 4), (2, 4), (2, 4)), 4, mine, other, core_two, core_three)
    weights = [*near, *coarse]

    one_a, a = first(a)
    for bit in range(1, narrow_bits):
        b = columns_step(b, bit)
    two_a, a = second(a, ())
    a, a_sent = third(one_a, two_a, a, ())
    one_b, b = first(b)
    a = grown(a, swapped(a_sent, "wide", 0))
    two_b, b = second(b, ())
    for bit in reversed(range(1, narrow_bits)):
        a = grown(a, swapped(a, "narrow", bit))
    b, b_sent = third(one_b, two_b, b, ())
    b = grown(b, swapped(b_sent, "wide", 0))
    out = finish(0, solved_a, a, swapped(a, "narrow", 0), [])
    for bit in reversed(range(1, narrow_bits)):
        b = grown(b, swapped(b, "narrow", bit))
    return finish(1, solved_b, b, swapped(b, "narrow", 0), [out])


def solution(mesh):
    placed = (
        P(None, ("wide", "narrow"), None),
        P(None, ("wide", "narrow"), None),
        P(None, ("wide", "narrow"), None),
        P(None, ("wide", "narrow"), None),
        P(None, "wide", None),
        P(None, ("wide", "narrow"), None),
        P(None, ("wide", "narrow"), None),
        P(),
        P(None, ("wide", "narrow"), None),
        P(None, ("wide", "narrow"), None),
        P(),
    )

    return jax.shard_map(
        body,
        mesh=mesh,
        in_specs=placed,
        out_specs=P(None, ("wide", "narrow"), None),
        check_vma=False,
    )
```
